32 devices in a mesh: fsdp: 8 (over y, x, core), seq: 4 (over z).
Axes of the slice: x: 2, y: 2, z: 4, core: 2. Of those that a mesh axis runs over, the one named last changes fastest.
Arguments:
- layer_input: bfloat16 [8, 512, 4096], P('fsdp', 'seq'), may hold values from -6 to 6
- dt_weight: bfloat16 [4096, 64], P('fsdp'), may hold values from -0.09375 to 0.09375
- dt_bias: float32 [64], replicated, may hold values from -2 to -0.5
- decay_rate: float32 [64], replicated, may hold values from 0.0005 to 0.25
- ssm_input: bfloat16 [8, 512, 2048], P('fsdp', 'seq'), may hold values from -6 to 6
- in_basis: bfloat16 [8, 512, 512], P('fsdp', 'seq'), may hold values from -0.59765625 to 0.59765625
- out_basis: bfloat16 [8, 512, 512], P('fsdp', 'seq'), may hold values from -0.59765625 to 0.59765625
- out_cotangent: bfloat16 [8, 512, 2048], P('fsdp', 'seq'), may hold values from -6 to 6
Outputs:
- grad_input: bfloat16 [8, 512, 2048], P('fsdp', 'seq')
- grad_in_basis: bfloat16 [8, 512, 512], P('fsdp', 'seq')
- grad_out_basis: bfloat16 [8, 512, 512], P('fsdp', 'seq')
- grad_dt_weight: float32 [4096, 64], P('fsdp')
The draws below stay inside these ranges and needn't reach their ends.
All inputs are finite; a program needn't handle non-finite values.
Results may differ from the reference program's by a relative error of at most 0.011.
Values may be sent and summed in bfloat16 or wider, within the bound.
A program may use at most 64 MiB of HBM per device.

```python
import math
import jax
import jax.numpy as jnp
from jax import lax

D = 4096
HEADS = 64
HEAD_DIM = 32
GROUPS = 4
STATE = 128
TOK_DEV = 128
SEQLEN = 512
BATCH = 8
N_SEQ = 4


def raised(values, key, source, target, parts, factor):
    owner, partner = [(jnp.arange(values.shape[dim]) // (values.shape[dim] // parts)).reshape([-1 if axis == dim else 1 for axis in range(values.ndim)]) for dim in (source, target)]
    chosen = jax.random.permutation(key, parts)[partner]
    strong = (owner == chosen) | (owner == (partner + parts // 2) % parts)
    return jnp.where(strong, factor * values, values)


def level_of(rng, extent, split, low, largest):
    factor_of = 1.0
    for dim, shards_of in split:
        heights = jax.random.uniform(jax.random.fold_in(jax.random.fold_in(rng, 6), dim), (shards_of,), jnp.float32, low / len(split), largest / len(split))
        factor_of = factor_of * jnp.repeat(jnp.exp(heights), extent[dim] // shards_of).reshape((-1,) + (1,) * (len(extent) - 1 - dim))
    return factor_of


def bell_draw(key, extent, scale, reach, cuts=(), dtype=jnp.bfloat16):
    entries = jax.random.normal(key, extent, jnp.float32) * scale
    if len(cuts) > 0:
        entries = level_of(key, extent, cuts, -0.22, 0.18) * entries
    return jnp.clip(entries, min=-reach, max=reach).astype(dtype)


def gaussian_with(own_key, shape, scale, most, shards, heavy, held_as=jnp.bfloat16):
    array = scale * jax.random.normal(own_key, shape, jnp.float32)
    if shards:
        array = array * level_of(own_key, shape, shards, -0.22, 0.18)
    return jnp.clip(raised(array, jax.random.fold_in(own_key, 3), *heavy), -most, most).astype(held_as)


def setup_inputs(seed: int = 0) -> dict:
    streams_of = jax.random.split(jax.random.key(seed), 9)
    layer_input = gaussian_with(streams_of[0], (BATCH, SEQLEN, D), 1.0, 6.0, ((0, 8), (1, 4)), (0, 2, 8, 2.0))
    dt_weight = bell_draw(streams_of[1], (D, HEADS), D ** -0.5, 0.09375, ((0, 8),))
    dt_bias = jnp.clip(jax.random.uniform(streams_of[2], (HEADS,), jnp.float32, -2.0, -0.5), -2.0, -0.5)
    decay_rate = jnp.clip(jnp.exp(jax.random.uniform(streams_of[3], (HEADS,), jnp.float32, math.log(0.0005), math.log(0.25))), 0.0005, 0.25)
    ssm_input = bell_draw(streams_of[4], (BATCH, SEQLEN, HEADS * HEAD_DIM), 1.0, 6.0, ((0, 8), (1, 4)))
    in_basis = bell_draw(streams_of[5], (BATCH, SEQLEN, GROUPS * STATE), 0.09, 0.59765625, ((0, 8), (1, 4)))
    out_basis = bell_draw(streams_of[6], (BATCH, SEQLEN, GROUPS * STATE), 0.09, 0.59765625, ((0, 8), (1, 4)))
    out_cotangent = bell_draw(streams_of[7], (BATCH, SEQLEN, HEADS * HEAD_DIM), 1.0, 6.0, ((0, 8), (1, 4)))
    return {"layer_input": layer_input, "dt_weight": dt_weight, "dt_bias": dt_bias, "decay_rate": decay_rate, "ssm_input": ssm_input, "in_basis": in_basis, "out_basis": out_basis, "out_cotangent": out_cotangent}


HIGH = lax.Precision.HIGHEST

def block_step(state, pieces):
    logdecay, step_size, inputs, basis_in, basis_out = pieces
    cumulative = jnp.cumsum(logdecay, axis=0)
    final = cumulative[-1]
    rows_first = cumulative.T
    spread = rows_first[:, :, None] - rows_first[:, None, :]
    position = jnp.arange(logdecay.shape[0])
    lower = position[:, None] >= position[None, :]
    decay_mat = jnp.where(lower, jnp.exp(jnp.where(lower, spread, 0.0)), 0.0)
    intersection = jnp.einsum('thn,shn->hts', basis_out, basis_in, precision=HIGH)
    weighted = decay_mat * intersection
    inner = jnp.einsum('hts,sh,shp->thp', weighted, step_size, inputs, precision=HIGH)
    from_state = jnp.exp(cumulative)[:, :, None] * jnp.einsum('hpn,thn->thp', state, basis_out, precision=HIGH)
    tail = jnp.exp(final[None, :] - cumulative) * step_size
    new_state = jnp.exp(final)[:, None, None] * state + jnp.einsum('sh,shp,shn->hpn', tail, inputs, basis_in, precision=HIGH)
    return (new_state, inner + from_state)

def forward(weight, inputs, basis_in, basis_out, tokens, dt_bias, decay_rate):
    raw = jnp.dot(tokens, weight, precision=HIGH) + dt_bias
    step_size = jax.nn.softplus(raw)
    logdecay = -decay_rate * step_size
    per_group = HEADS // GROUPS
    inputs_h = inputs.reshape(N_SEQ, TOK_DEV, HEADS, HEAD_DIM)
    bin_h = jnp.repeat(basis_in.reshape(N_SEQ, TOK_DEV, GROUPS, STATE), per_group, axis=2)
    bout_h = jnp.repeat(basis_out.reshape(N_SEQ, TOK_DEV, GROUPS, STATE), per_group, axis=2)
    start = jnp.zeros((HEADS, HEAD_DIM, STATE), jnp.float32)
    pieces = (logdecay.reshape(N_SEQ, TOK_DEV, HEADS), step_size.reshape(N_SEQ, TOK_DEV, HEADS), inputs_h, bin_h, bout_h)
    _, outputs = lax.scan(block_step, start, pieces)
    return outputs.reshape(N_SEQ * TOK_DEV, HEADS * HEAD_DIM)

def reference(layer_input, dt_weight, dt_bias, decay_rate, ssm_input, in_basis, out_basis, out_cotangent):
    weight = dt_weight.astype(jnp.float32)

    def one_sequence(total, row):
        tokens, inputs, basis_in, basis_out, upstream = row
        tokens = tokens.astype(jnp.float32)

        def local(wmat, xval, bval, cval):
            return forward(wmat, xval, bval, cval, tokens, dt_bias, decay_rate)
        _, pull = jax.vjp(local, weight, inputs.astype(jnp.float32), basis_in.astype(jnp.float32), basis_out.astype(jnp.float32))
        grad_w, grad_x, grad_b, grad_c = pull(upstream.astype(jnp.float32))
        return (total + grad_w, (grad_x.astype(jnp.bfloat16), grad_b.astype(jnp.bfloat16), grad_c.astype(jnp.bfloat16)))
    start = jnp.zeros((D, HEADS), jnp.float32)
    total, (grad_x, grad_b, grad_c) = lax.scan(one_sequence, start, (layer_input, ssm_input, in_basis, out_basis, out_cotangent))
    return (grad_x, grad_b, grad_c, total)
```

```python
import functools

import jax
import jax.numpy as jnp
from jax import lax
from jax.experimental import pallas as pl
from jax.experimental.pallas import tpu as pltpu
from jax.sharding import PartitionSpec as P

STATE = 128
F32 = jnp.float32
BF16 = jnp.bfloat16
MESH = pl.DeviceIdType.MESH
HIGH = lax.Precision.HIGHEST


def dot(a, b, ca=1, cb=0, precision=None):
    return lax.dot_general(
        a, b, (((ca,), (cb,)), ((), ())), precision=precision, preferred_element_type=F32
    )


def halves(value, axis):
    high = value.astype(BF16)
    low = (value - high.astype(F32)).astype(BF16)
    return jnp.concatenate([high, low], axis=axis)


def iota(shape, dim):
    return lax.broadcasted_iota(jnp.int32, shape, dim)


def reverse_bits(value, bits):
    return sum(((value // 2**j) % 2) * 2 ** (bits - 1 - j) for j in range(bits))


def kernel(
    nf,
    ns,
    tokens,
    weight_t,
    bias,
    rate_row,
    x,
    b_in,
    c_out,
    dy,
    out_x,
    out_b,
    out_c,
    out_w,
    gathered,
    raw_t,
    cum_t,
    step_t,
    block_t,
    cum_g,
    step_g,
    tail_g,
    lead_g,
    state_loc,
    grad_loc,
    xs_g,
    ds_g,
    entry,
    later,
    send_f,
    send_b,
    through,
    grad_b,
    grad_c,
    col_t,
    xt_t,
    xc_t,
    ent_t,
    total,
    rs_send,
    rs_recv,
    z_recv,
    ag_ssem,
    ag_rsem,
    f_ssem,
    f_rsem,
    b_ssem,
    b_rsem,
    rs_ssem,
    rs_rsem,
    z_ssem,
    z_rsem,
):
    f = lax.axis_index("fsdp")
    z = lax.axis_index("seq")
    length = tokens.shape[0]
    heads, rows = weight_t.shape
    groups = b_in.shape[1] // STATE
    per = heads // groups
    wide = x.shape[1] // groups
    size = wide // per
    bits = nf.bit_length() - 1

    def partner(j):
        return f + (1 - 2 * ((f // 2**j) % 2)) * 2**j

    barrier = pltpu.get_barrier_semaphore()
    for j in range(bits):
        pl.semaphore_signal(
            barrier, inc=1, device_id={"fsdp": partner(j)}, device_id_type=MESH
        )
    for d in range(1, ns):
        pl.semaphore_signal(
            barrier, inc=1, device_id={"seq": (z + d) % ns}, device_id_type=MESH
        )
    pl.semaphore_wait(barrier, bits + ns - 1)

    slot = reverse_bits(f, bits)
    gathered[slot] = weight_t[...]
    for i in range(bits):
        j = bits - 1 - i
        part = gathered.at[pl.ds((slot // 2**i) * 2**i, 2**i)]
        copy = pltpu.make_async_remote_copy(
            src_ref=part,
            dst_ref=part,
            send_sem=ag_ssem.at[i],
            recv_sem=ag_rsem.at[i],
            device_id={"fsdp": partner(j)},
            device_id_type=MESH,
        )
        copy.start()
        copy.wait()

    raw = jnp.broadcast_to(bias[...], (length, heads)).T
    rate = jnp.broadcast_to(rate_row[...], (length, heads)).T
    for s in range(nf):
        own = reverse_bits(s, bits)
        raw = raw + dot(gathered[s], tokens[:, own * rows : (own + 1) * rows], 1, 1)
    step = jnp.maximum(raw, 0.0) + jnp.log1p(jnp.exp(-jnp.abs(raw)))
    before = iota((length, length), 0) <= iota((length, length), 1)
    cum = dot(-rate * step, before.astype(F32), precision=HIGH)
    raw_t[...] = raw
    cum_t[...] = cum
    step_t[...] = step
    final = cum[:, length - 1 : length]
    block_t[...] = jnp.broadcast_to(jnp.exp(final), (heads, STATE))
    both = jnp.concatenate([cum, step], axis=0).T
    cum_c = both[:, :heads]
    step_c = both[:, heads:]
    tail_c = jnp.exp(cum_c[length - 1 : length] - cum_c)
    lead_c = jnp.exp(cum_c)
    for g in range(groups):
        span = slice(g * per, (g + 1) * per)
        cum_g[g] = cum_c[:, span]
        step_g[g] = step_c[:, span]
        tail_g[g] = tail_c[:, span]
        lead_g[g] = lead_c[:, span]

    spread_one = (iota((2 * per, wide), 0) % per == iota((2 * per, wide), 1) // size).astype(BF16)
    gather_one = (iota((per, wide), 0) == iota((per, wide), 1) // size).astype(BF16)

    def expand(value):
        return dot(halves(value, 1), spread_one)

    def head_sums(value):
        high = value.astype(BF16)
        low = (value - high.astype(F32)).astype(BF16)
        return dot(gather_one, high, 1, 1) + dot(gather_one, low, 1, 1)

    def span_of(g, width):
        return pl.ds(pl.multiple_of(g * width, width), width)

    @pl.when(z == 0)
    def _():
        entry[...] = jnp.zeros_like(entry)

    @pl.when(z == ns - 1)
    def _():
        later[...] = jnp.zeros_like(later)

    def forward_copy(g):
        return pltpu.make_async_remote_copy(
            src_ref=send_f.at[g],
            dst_ref=entry.at[g],
            send_sem=f_ssem.at[g],
            recv_sem=f_rsem.at[g],
            device_id={"seq": (z + 1) % ns},
            device_id_type=MESH,
        )

    def backward_copy(g):
        return pltpu.make_async_remote_copy(
            src_ref=send_b.at[g],
            dst_ref=later.at[g],
            send_sem=b_ssem.at[g],
            recv_sem=b_rsem.at[g],
            device_id={"seq": (z + ns - 1) % ns},
            device_id_type=MESH,
        )

    def local(g):
        xs = (x[:, span_of(g, wide)].astype(F32) * expand(step_g[g] * tail_g[g])).astype(BF16)
        ds = (dy[:, span_of(g, wide)].astype(F32) * expand(lead_g[g])).astype(BF16)
        xs_g[g] = xs
        ds_g[g] = ds
        state_loc[g] = dot(xs, b_in[:, span_of(g, STATE)], 0, 0)
        grad_loc[g] = dot(ds, c_out[:, span_of(g, STATE)], 0, 0)

    def decay_rows(g):
        return dot(spread_one, halves(block_t[span_of(g, per)], 0), 0, 0)

    def chain_f(g):
        @pl.when(z > 0)
        def _():
            forward_copy(g).wait_recv()

        @pl.when(z < ns - 1)
        def _():
            send_f[g] = (decay_rows(g) * entry[g].astype(F32) + state_loc[g]).astype(BF16)
            forward_copy(g).start()

    def chain_b(g):
        @pl.when(z < ns - 1)
        def _():
            backward_copy(g).wait_recv()

        @pl.when(z > 0)
        def _():
            send_b[g] = (decay_rows(g) * later[g].astype(F32) + grad_loc[g]).astype(BF16)
            backward_copy(g).start()

    def heavy(g):
        inputs = x[:, span_of(g, wide)]
        upstream = dy[:, span_of(g, wide)]
        b = b_in[:, span_of(g, STATE)]
        c = c_out[:, span_of(g, STATE)]
        meet = dot(b, c, 1, 1)
        upper = iota((length, length), 0) <= iota((length, length), 1)
        lanes = iota((length, 128), 1)
        cum_r = cum_t[span_of(g, per)]
        cum_l = cum_g[g]
        step_l = step_g[g]
        joint = jnp.zeros((length, length), F32)
        sums = []
        pieces = []
        for q in range(wide // 128):
            x_q = inputs[:, q * 128 : (q + 1) * 128]
            dy_q = upstream[:, q * 128 : (q + 1) * 128]
            weights = []
            masked = []
            for j in range(128 // size):
                k = q * (128 // size) + j
                mine = lanes // size == j
                pair = dot(jnp.where(mine, x_q, jnp.zeros_like(x_q)), dy_q, 1, 1)
                spread = cum_r[k : k + 1] - cum_l[:, k : k + 1]
                decay = jnp.exp(jnp.where(upper, spread, -1e30))
                weights.append((decay * meet).astype(BF16))
                masked.append(jnp.where(mine, dy_q, jnp.zeros_like(dy_q)))
                scaled = decay * pair * step_l[:, k : k + 1]
                joint = joint + scaled
                sums.append(jnp.sum(scaled * meet, axis=0, keepdims=True))
            pieces.append(
                dot(jnp.concatenate(weights, axis=1), jnp.concatenate(masked, axis=0))
            )
        passed = jnp.concatenate(pieces, axis=1)
        through[g] = passed
        col_t[span_of(g, per)] = jnp.concatenate(sums, axis=0)
        xt_t[span_of(g, per)] = head_sums(inputs.astype(F32) * passed)
        joint = joint.astype(BF16)
        grad_b[g] = dot(joint, c)
        grad_c[g] = dot(joint, b, 0, 0)

    def finish_f(g):
        c = c_out[:, span_of(g, STATE)]
        read = dot(c, entry[g], 1, 1)
        ent_t[span_of(g, per)] = head_sums(ds_g[g].astype(F32) * read)
        out_c[:, span_of(g, STATE)] = (grad_c[g] + dot(ds_g[g], entry[g])).astype(BF16)

    def finish_b(g):
        b = b_in[:, span_of(g, STATE)]
        carried = dot(b, later[g], 1, 1)
        xc_t[span_of(g, per)] = head_sums(x[:, span_of(g, wide)].astype(F32) * carried)
        inner = through[g] + expand(tail_g[g]) * carried
        out_x[:, span_of(g, wide)] = (expand(step_g[g]) * inner).astype(BF16)
        out_b[:, span_of(g, STATE)] = (grad_b[g] + dot(xs_g[g], later[g])).astype(BF16)

    def within(g):
        return jnp.logical_and(g >= 0, g < groups)

    def slot_step(tau, carry):
        gf = tau - z
        gb = tau - (ns - 1 - z)
        pl.when(tau < groups)(lambda: local(tau))
        pl.when(within(gf))(lambda: chain_f(gf))
        pl.when(within(gb))(lambda: chain_b(gb))
        pl.when(tau < groups)(lambda: heavy(tau))
        pl.when(within(gf))(lambda: finish_f(gf))
        pl.when(within(gb))(lambda: finish_b(gb))
        return carry

    lax.fori_loop(0, groups + ns - 1, slot_step, 0)

    crossing = jnp.concatenate(
        [
            dot(gather_one, (entry[g].astype(F32) * later[g].astype(F32)).astype(BF16))
            for g in range(groups)
        ],
        axis=0,
    )
    cum = cum_t[...]
    step = step_t[...]
    raw = raw_t[...]
    tail = jnp.exp(cum[:, length - 1 : length] - cum)
    xt = xt_t[...]
    tail_xc = tail * xc_t[...]
    leaving = step * tail_xc
    grad_cum = col_t[...] - step * xt + ent_t[...] - leaving
    closing = block_t[:, :1] * jnp.sum(crossing, axis=1, keepdims=True) + jnp.sum(
        leaving, axis=1, keepdims=True
    )
    after = (iota((length, length), 0) >= iota((length, length), 1)).astype(F32)
    grad_log = dot(grad_cum, after, precision=HIGH) + closing
    grad_raw = (xt + tail_xc - rate * grad_log) * jax.nn.sigmoid(raw)
    grad_raw = grad_raw.astype(BF16)

    base = 0
    count = nf
    for j in range(bits):
        bit = (f // 2**j) % 2
        half = count // 2
        if j == 0 and rows % 128 == 0:
            for i in range(half):
                own = 2 * i + (1 - bit)
                columns = pl.ds(pl.multiple_of(own * rows, 128), rows)
                rs_send[i_slot(i, bits)] = dot(grad_raw, tokens[:, columns]).astype(BF16)
        else:
            if j == 0:
                for s in range(nf):
                    own = reverse_bits(s, bits)
                    total[s] = dot(grad_raw, tokens[:, own * rows : (own + 1) * rows])
            rs_send[pl.ds(nf - count, half)] = total[
                pl.ds(base + (1 - bit) * half, half)
            ].astype(BF16)
        copy = pltpu.make_async_remote_copy(
            src_ref=rs_send.at[pl.ds(nf - count, half)],
            dst_ref=rs_recv.at[pl.ds(nf - count, half)],
            send_sem=rs_ssem.at[j],
            recv_sem=rs_rsem.at[j],
            device_id={"fsdp": partner(j)},
            device_id_type=MESH,
        )
        copy.start()
        if j == 0 and rows % 128 == 0:
            for i in range(half):
                own = 2 * i + bit
                columns = pl.ds(pl.multiple_of(own * rows, 128), rows)
                total[bit * half + i_slot(i, bits)] = dot(grad_raw, tokens[:, columns])
        copy.wait()
        base = base + bit * half
        total[pl.ds(base, half)] += rs_recv[pl.ds(nf - count, half)].astype(F32)
        count = half

    z_recv[z] = total[base].astype(BF16)
    copies = []
    for d in range(1, ns):
        copy = pltpu.make_async_remote_copy(
            src_ref=z_recv.at[z],
            dst_ref=z_recv.at[z],
            send_sem=z_ssem.at[d - 1],
            recv_sem=z_rsem.at[d - 1],
            device_id={"seq": (z + d) % ns},
            device_id_type=MESH,
        )
        copy.start()
        copies.append(copy)
    for copy in copies:
        copy.wait()
    summed = z_recv[0].astype(F32)
    for k in range(1, ns):
        summed = summed + z_recv[k].astype(F32)
    out_w[...] = summed

    @pl.when(z < ns - 1)
    def _():
        for g in range(groups):
            forward_copy(g).wait_send()

    @pl.when(z > 0)
    def _():
        for g in range(groups):
            backward_copy(g).wait_send()


def i_slot(i, bits):
    return reverse_bits(i, bits - 1)


def body(
    layer_input, dt_weight, dt_bias, decay_rate, ssm_input, in_basis, out_basis, out_cotangent
):
    nf, ns = lax.axis_size("fsdp"), lax.axis_size("seq")
    length = layer_input.shape[1]
    rows, heads = dt_weight.shape
    groups = in_basis.shape[2] // STATE
    per = heads // groups
    full = ssm_input.shape[2]
    wide = full // groups
    bits = nf.bit_length() - 1
    tall = (groups, wide, STATE)
    dma = pltpu.SemaphoreType.DMA
    v = pltpu.VMEM
    scratch = [
        v((nf, heads, rows), BF16),
        v((heads, length), F32),
        v((heads, length), F32),
        v((heads, length), F32),
        v((heads, STATE), F32),
        v((groups, length, per), F32),
        v((groups, length, per), F32),
        v((groups, length, per), F32),
        v((groups, length, per), F32),
        v(tall, F32),
        v(tall, F32),
        v((groups, length, wide), BF16),
        v((groups, length, wide), BF16),
        v(tall, BF16),
        v(tall, BF16),
        v(tall, BF16),
        v(tall, BF16),
        v((groups, length, wide), F32),
        v((groups, length, STATE), F32),
        v((groups, length, STATE), F32),
        v((heads, length), F32),
        v((heads, length), F32),
        v((heads, length), F32),
        v((heads, length), F32),
        v((nf, heads, rows), F32),
        v((nf, heads, rows), BF16),
        v((nf, heads, rows), BF16),
        v((ns, heads, rows), BF16),
        dma((bits,)),
        dma((bits,)),
        dma((groups,)),
        dma((groups,)),
        dma((groups,)),
        dma((groups,)),
        dma((bits,)),
        dma((bits,)),
        dma((ns - 1,)),
        dma((ns - 1,)),
    ]
    out_x, out_b, out_c, out_w = pl.pallas_call(
        functools.partial(kernel, nf, ns),
        out_shape=(
            jax.ShapeDtypeStruct((length, full), BF16),
            jax.ShapeDtypeStruct((length, groups * STATE), BF16),
            jax.ShapeDtypeStruct((length, groups * STATE), BF16),
            jax.ShapeDtypeStruct((heads, rows), F32),
        ),
        in_specs=[pl.BlockSpec(memory_space=pltpu.VMEM)] * 8,
        out_specs=[pl.BlockSpec(memory_space=pltpu.VMEM)] * 4,
        scratch_shapes=scratch,
        compiler_params=pltpu.CompilerParams(
            collective_id=0, has_side_effects=True, vmem_limit_bytes=60 * 1024 * 1024
        ),
    )(
        layer_input[0],
        dt_weight.T,
        dt_bias[None],
        decay_rate[None],
        ssm_input[0],
        in_basis[0],
        out_basis[0],
        out_cotangent[0],
    )
    return (out_x[None], out_b[None], out_c[None], out_w.T)


def solution(mesh):
    blocks = P("fsdp", "seq", None)
    rows = P("fsdp", None)
    return jax.shard_map(
        body,
        mesh=mesh,
        in_specs=(blocks, rows, P(), P(), blocks, blocks, blocks, blocks),
        out_specs=(blocks, blocks, blocks, rows),
        check_vma=False,
    )
```

```python
import functools

import jax
import jax.numpy as jnp
from jax import lax
from jax.experimental import pallas as pl
from jax.experimental.pallas import tpu as pltpu
from jax.sharding import PartitionSpec as P

STATE = 128
F32 = jnp.float32
BF16 = jnp.bfloat16
MESH = pl.DeviceIdType.MESH
HIGH = lax.Precision.HIGHEST


def dot(a, b, ca=1, cb=0, precision=None):
    return lax.dot_general(
        a, b, (((ca,), (cb,)), ((), ())), precision=precision, preferred_element_type=F32
    )


def halves(value, axis):
    high = value.astype(BF16)
    low = (value - high.astype(F32)).astype(BF16)
    return jnp.concatenate([high, low], axis=axis)


def iota(shape, dim):
    return lax.broadcasted_iota(jnp.int32, shape, dim)


def kernel(
    nf,
    ns,
    tokens_hbm,
    weight_t,
    bias,
    rate_row,
    x_hbm,
    b_hbm,
    c_hbm,
    dy_hbm,
    x_out,
    b_out,
    c_out_hbm,
    out_w,
    tokens,
    x,
    b_in,
    c_out,
    dy,
    out_x,
    out_b,
    out_c,
    in_sem,
    out_sem,
    gathered,
    raw_t,
    cum_t,
    step_t,
    block_t,
    cum_g,
    step_g,
    tail_g,
    lead_g,
    state_loc,
    grad_loc,
    xs_g,
    ds_g,
    entry,
    later,
    send_f,
    send_b,
    through,
    grad_b,
    grad_c,
    col_t,
    xt_t,
    xc_t,
    ent_t,
    total,
    rs_send,
    rs_recv,
    z_recv,
    ag_ssem,
    ag_rsem,
    f_ssem,
    f_rsem,
    b_ssem,
    b_rsem,
    rs_ssem,
    rs_rsem,
    z_ssem,
    z_rsem,
):
    f = lax.axis_index("fsdp")
    z = lax.axis_index("seq")
    length = tokens.shape[0]
    heads, rows = weight_t.shape
    groups = b_in.shape[1] // STATE
    per = heads // groups
    wide = x.shape[1] // groups
    size = wide // per
    bits = nf.bit_length() - 1
    part_heads = heads // 2
    chunk = wide // 2
    loads = [
        pltpu.make_async_copy(source, target, in_sem.at[n])
        for n, (source, target) in enumerate(
            (
                (tokens_hbm, tokens),
                (x_hbm, x),
                (dy_hbm, dy),
                (b_hbm, b_in),
                (c_hbm, c_out),
            )
        )
    ]
    for load in loads:
        load.start()
    orders = (list(reversed(range(bits))), list(range(1, bits)) + [0])

    def slot_of(index, order):
        return sum(((index // 2**b) % 2) * 2**i for i, b in enumerate(order))

    def partner(j):
        return f + (1 - 2 * ((f // 2**j) % 2)) * 2**j

    barrier = pltpu.get_barrier_semaphore()
    for j in range(bits):
        pl.semaphore_signal(
            barrier, inc=1, device_id={"fsdp": partner(j)}, device_id_type=MESH
        )
    for d in range(1, ns):
        pl.semaphore_signal(
            barrier, inc=1, device_id={"seq": (z + d) % ns}, device_id_type=MESH
        )
    pl.semaphore_wait(barrier, bits + ns - 1)

    slots = [slot_of(f, order) for order in orders]
    for h in range(2):
        gathered[h, slots[h]] = weight_t[h * part_heads : (h + 1) * part_heads]
    for i in range(bits):
        copies = []
        for h in range(2):
            part = gathered.at[h, pl.ds((slots[h] // 2**i) * 2**i, 2**i)]
            copy = pltpu.make_async_remote_copy(
                src_ref=part,
                dst_ref=part,
                send_sem=ag_ssem.at[h, i],
                recv_sem=ag_rsem.at[h, i],
                device_id={"fsdp": partner(orders[h][i])},
                device_id_type=MESH,
            )
            copy.start()
            copies.append(copy)
        if i == bits - 1:
            for load in loads:
                load.wait()
        for copy in copies:
            copy.wait()

    raw = jnp.broadcast_to(bias[...], (length, heads)).T
    rate = jnp.broadcast_to(rate_row[...], (length, heads)).T
    for own in range(nf):
        weight = jnp.concatenate(
            [gathered[h, slot_of(own, orders[h])] for h in range(2)], axis=0
        )
        raw = raw + dot(weight, tokens[:, own * rows : (own + 1) * rows], 1, 1)
    step = jnp.maximum(raw, 0.0) + jnp.log1p(jnp.exp(-jnp.abs(raw)))
    before = iota((length, length), 0) <= iota((length, length), 1)
    cum = dot(-rate * step, before.astype(F32), precision=HIGH)
    raw_t[...] = raw
    cum_t[...] = cum
    step_t[...] = step
    final = cum[:, length - 1 : length]
    block_t[...] = jnp.broadcast_to(jnp.exp(final), (heads, STATE))
    both = jnp.concatenate([cum, step], axis=0).T
    cum_c = both[:, :heads]
    step_c = both[:, heads:]
    tail_c = jnp.exp(cum_c[length - 1 : length] - cum_c)
    lead_c = jnp.exp(cum_c)
    for g in range(groups):
        span = slice(g * per, (g + 1) * per)
        cum_g[g] = cum_c[:, span]
        step_g[g] = step_c[:, span]
        tail_g[g] = tail_c[:, span]
        lead_g[g] = lead_c[:, span]

    spread_one = (iota((2 * per, wide), 0) % per == iota((2 * per, wide), 1) // size).astype(BF16)
    gather_one = (iota((per, wide), 0) == iota((per, wide), 1) // size).astype(BF16)

    def expand(value):
        return dot(halves(value, 1), spread_one)

    def head_sums(value):
        high = value.astype(BF16)
        low = (value - high.astype(F32)).astype(BF16)
        return dot(gather_one, high, 1, 1) + dot(gather_one, low, 1, 1)

    def span_of(g, width):
        return pl.ds(pl.multiple_of(g * width, width), width)

    @pl.when(z == 0)
    def _():
        entry[...] = jnp.zeros_like(entry)

    @pl.when(z == ns - 1)
    def _():
        later[...] = jnp.zeros_like(later)

    spread_half = (
        iota((per, chunk), 0) % (per // 2) == iota((per, chunk), 1) // size
    ).astype(BF16)

    def piece(g):
        return g // 2, pl.ds(pl.multiple_of((g % 2) * chunk, chunk), chunk)

    def forward_copy(g):
        return pltpu.make_async_remote_copy(
            src_ref=send_f.at[piece(g)],
            dst_ref=entry.at[piece(g)],
            send_sem=f_ssem.at[g],
            recv_sem=f_rsem.at[g],
            device_id={"seq": (z + 1) % ns},
            device_id_type=MESH,
        )

    def backward_copy(g):
        return pltpu.make_async_remote_copy(
            src_ref=send_b.at[piece(g)],
            dst_ref=later.at[piece(g)],
            send_sem=b_ssem.at[g],
            recv_sem=b_rsem.at[g],
            device_id={"seq": (z + ns - 1) % ns},
            device_id_type=MESH,
        )

    def local(g):
        xs = (x[:, span_of(g, wide)].astype(F32) * expand(step_g[g] * tail_g[g])).astype(BF16)
        ds = (dy[:, span_of(g, wide)].astype(F32) * expand(lead_g[g])).astype(BF16)
        xs_g[g] = xs
        ds_g[g] = ds
        state_loc[g] = dot(xs, b_in[:, span_of(g, STATE)], 0, 0)
        grad_loc[g] = dot(ds, c_out[:, span_of(g, STATE)], 0, 0)

    def decay_rows(g):
        return dot(spread_half, halves(block_t[span_of(g, per // 2)], 0), 0, 0)

    def chain_f(g):
        @pl.when(z > 0)
        def _():
            forward_copy(g).wait_recv()

        @pl.when(z < ns - 1)
        def _():
            p = piece(g)
            send_f[p] = (decay_rows(g) * entry[p].astype(F32) + state_loc[p]).astype(BF16)
            forward_copy(g).start()

    def chain_b(g):
        @pl.when(z < ns - 1)
        def _():
            backward_copy(g).wait_recv()

        @pl.when(z > 0)
        def _():
            p = piece(g)
            send_b[p] = (decay_rows(g) * later[p].astype(F32) + grad_loc[p]).astype(BF16)
            backward_copy(g).start()

    def heavy(g):
        inputs = x[:, span_of(g, wide)]
        upstream = dy[:, span_of(g, wide)]
        b = b_in[:, span_of(g, STATE)]
        c = c_out[:, span_of(g, STATE)]
        meet = dot(b, c, 1, 1)
        upper = iota((length, length), 0) <= iota((length, length), 1)
        lanes = iota((length, 128), 1)
        cum_r = cum_t[span_of(g, per)]
        cum_l = cum_g[g]
        step_l = step_g[g]
        joint = jnp.zeros((length, length), F32)
        sums = []
        pieces = []
        for q in range(wide // 128):
            x_q = inputs[:, q * 128 : (q + 1) * 128]
            dy_q = upstream[:, q * 128 : (q + 1) * 128]
            weights = []
            masked = []
            for j in range(128 // size):
                k = q * (128 // size) + j
                mine = lanes // size == j
                pair = dot(jnp.where(mine, x_q, jnp.zeros_like(x_q)), dy_q, 1, 1)
                spread = cum_r[k : k + 1] - cum_l[:, k : k + 1]
                decay = jnp.exp(jnp.where(upper, spread, -1e30))
                weights.append((decay * meet).astype(BF16))
                masked.append(jnp.where(mine, dy_q, jnp.zeros_like(dy_q)))
                scaled = decay * pair * step_l[:, k : k + 1]
                joint = joint + scaled
                sums.append(jnp.sum(scaled * meet, axis=0, keepdims=True))
            pieces.append(
                dot(jnp.concatenate(weights, axis=1), jnp.concatenate(masked, axis=0))
            )
        passed = jnp.concatenate(pieces, axis=1)
        through[g] = passed
        col_t[span_of(g, per)] = jnp.concatenate(sums, axis=0)
        xt_t[span_of(g, per)] = head_sums(inputs.astype(F32) * passed)
        joint = joint.astype(BF16)
        grad_b[g] = dot(joint, c)
        grad_c[g] = dot(joint, b, 0, 0)

    def finish_f(g):
        c = c_out[:, span_of(g, STATE)]
        read = dot(c, entry[g], 1, 1)
        ent_t[span_of(g, per)] = head_sums(ds_g[g].astype(F32) * read)
        out_c[:, span_of(g, STATE)] = (grad_c[g] + dot(ds_g[g], entry[g])).astype(BF16)

    def finish_b(g):
        b = b_in[:, span_of(g, STATE)]
        carried = dot(b, later[g], 1, 1)
        xc_t[span_of(g, per)] = head_sums(x[:, span_of(g, wide)].astype(F32) * carried)
        inner = through[g] + expand(tail_g[g]) * carried
        out_x[:, span_of(g, wide)] = (expand(step_g[g]) * inner).astype(BF16)
        out_b[:, span_of(g, STATE)] = (grad_b[g] + dot(xs_g[g], later[g])).astype(BF16)

    def within(g):
        return jnp.logical_and(g >= 0, g < groups)

    def slot_step(tau, carry):
        gf = tau - z
        gb = tau - (ns - 1 - z)
        pl.when(tau < groups)(lambda: local(tau))
        pl.when(within(gf))(lambda: chain_f(2 * gf))
        pl.when(within(gb))(lambda: chain_b(2 * gb))
        pl.when(tau < groups)(lambda: heavy(tau))
        pl.when(within(gf))(lambda: chain_f(2 * gf + 1))
        pl.when(within(gb))(lambda: chain_b(2 * gb + 1))
        pl.when(within(gf))(lambda: finish_f(gf))
        pl.when(within(gb))(lambda: finish_b(gb))
        return carry

    lax.fori_loop(0, groups + ns - 1, slot_step, 0)
    stores = [
        pltpu.make_async_copy(source, target, out_sem.at[n])
        for n, (source, target) in enumerate(
            ((out_x, x_out), (out_b, b_out), (out_c, c_out_hbm))
        )
    ]
    for store in stores:
        store.start()

    crossing = jnp.concatenate(
        [
            dot(gather_one, (entry[g].astype(F32) * later[g].astype(F32)).astype(BF16))
            for g in range(groups)
        ],
        axis=0,
    )
    cum = cum_t[...]
    step = step_t[...]
    raw = raw_t[...]
    tail = jnp.exp(cum[:, length - 1 : length] - cum)
    xt = xt_t[...]
    tail_xc = tail * xc_t[...]
    leaving = step * tail_xc
    grad_cum = col_t[...] - step * xt + ent_t[...] - leaving
    closing = block_t[:, :1] * jnp.sum(crossing, axis=1, keepdims=True) + jnp.sum(
        leaving, axis=1, keepdims=True
    )
    after = (iota((length, length), 0) >= iota((length, length), 1)).astype(F32)
    grad_log = dot(grad_cum, after, precision=HIGH) + closing
    grad_raw = (xt + tail_xc - rate * grad_log) * jax.nn.sigmoid(raw)
    grad_raw = grad_raw.astype(BF16)

    bases = [0, 0]
    count = nf
    early = rows % 128 == 0

    def product(own, target, place, offset):
        columns = pl.ds(pl.multiple_of(own * rows, 128), rows) if early else slice(
            own * rows, (own + 1) * rows
        )
        block = dot(grad_raw, tokens[:, columns])
        for h in range(2):
            target[h, offset + place[h]] = block[
                h * part_heads : (h + 1) * part_heads
            ].astype(target.dtype)

    for j in range(bits):
        half = count // 2
        sent = pl.ds(nf - count, half)
        if j == 0 and early:
            bit = f % 2
            for i in range(half):
                place = [slot_of(2 * i, order) for order in orders]
                product(2 * i + (1 - bit), rs_send, place, 0)
        elif j == 0:
            for own in range(nf):
                product(own, total, [slot_of(own, order) for order in orders], 0)
        copies = []
        for h in range(2):
            b = orders[h][bits - 1 - j]
            bit_h = (f // 2**b) % 2
            if j > 0 or not early:
                rs_send[h, sent] = total[
                    h, pl.ds(bases[h] + (1 - bit_h) * half, half)
                ].astype(BF16)
            copy = pltpu.make_async_remote_copy(
                src_ref=rs_send.at[h, sent],
                dst_ref=rs_recv.at[h, sent],
                send_sem=rs_ssem.at[h, j],
                recv_sem=rs_rsem.at[h, j],
                device_id={"fsdp": partner(b)},
                device_id_type=MESH,
            )
            copy.start()
            copies.append(copy)
            bases[h] = bases[h] + bit_h * half
        if j == 0 and early:
            for i in range(half):
                place = [slot_of(2 * i, order) for order in orders]
                product(2 * i + bit, total, place, bit * half)
        for h in range(2):
            copies[h].wait()
            total[h, pl.ds(bases[h], half)] += rs_recv[h, sent].astype(F32)
        count = half

    z_recv[z] = jnp.concatenate([total[h, bases[h]] for h in range(2)], axis=0).astype(BF16)
    copies = []
    for d in range(1, ns):
        copy = pltpu.make_async_remote_copy(
            src_ref=z_recv.at[z],
            dst_ref=z_recv.at[z],
            send_sem=z_ssem.at[d - 1],
            recv_sem=z_rsem.at[d - 1],
            device_id={"seq": (z + d) % ns},
            device_id_type=MESH,
        )
        copy.start()
        copies.append(copy)
    for copy in copies:
        copy.wait()
    summed = z_recv[0].astype(F32)
    for k in range(1, ns):
        summed = summed + z_recv[k].astype(F32)
    out_w[...] = summed

    @pl.when(z < ns - 1)
    def _():
        for g in range(2 * groups):
            forward_copy(g).wait_send()

    @pl.when(z > 0)
    def _():
        for g in range(2 * groups):
            backward_copy(g).wait_send()

    for store in stores:
        store.wait()


def body(
    layer_input, dt_weight, dt_bias, decay_rate, ssm_input, in_basis, out_basis, out_cotangent
):
    nf, ns = lax.axis_size("fsdp"), lax.axis_size("seq")
    length = layer_input.shape[1]
    rows, heads = dt_weight.shape
    groups = in_basis.shape[2] // STATE
    per = heads // groups
    full = ssm_input.shape[2]
    wide = full // groups
    bits = nf.bit_length() - 1
    tall = (groups, wide, STATE)
    dma = pltpu.SemaphoreType.DMA
    v = pltpu.VMEM
    scratch = [
        v((length, layer_input.shape[2]), BF16),
        v((length, full), BF16),
        v((length, groups * STATE), BF16),
        v((length, groups * STATE), BF16),
        v((length, full), BF16),
        v((length, full), BF16),
        v((length, groups * STATE), BF16),
        v((length, groups * STATE), BF16),
        dma((5,)),
        dma((3,)),
        v((2, nf, heads // 2, rows), BF16),
        v((heads, length), F32),
        v((heads, length), F32),
        v((heads, length), F32),
        v((heads, STATE), F32),
        v((groups, length, per), F32),
        v((groups, length, per), F32),
        v((groups, length, per), F32),
        v((groups, length, per), F32),
        v(tall, F32),
        v(tall, F32),
        v((groups, length, wide), BF16),
        v((groups, length, wide), BF16),
        v(tall, BF16),
        v(tall, BF16),
        v(tall, BF16),
        v(tall, BF16),
        v((groups, length, wide), F32),
        v((groups, length, STATE), F32),
        v((groups, length, STATE), F32),
        v((heads, length), F32),
        v((heads, length), F32),
        v((heads, length), F32),
        v((heads, length), F32),
        v((2, nf, heads // 2, rows), F32),
        v((2, nf, heads // 2, rows), BF16),
        v((2, nf, heads // 2, rows), BF16),
        v((ns, heads, rows), BF16),
        dma((2, bits)),
        dma((2, bits)),
        dma((2 * groups,)),
        dma((2 * groups,)),
        dma((2 * groups,)),
        dma((2 * groups,)),
        dma((2, bits)),
        dma((2, bits)),
        dma((ns - 1,)),
        dma((ns - 1,)),
    ]
    anywhere = pl.BlockSpec(memory_space=pl.ANY)
    inside = pl.BlockSpec(memory_space=pltpu.VMEM)
    out_x, out_b, out_c, out_w = pl.pallas_call(
        functools.partial(kernel, nf, ns),
        out_shape=(
            jax.ShapeDtypeStruct((length, full), BF16),
            jax.ShapeDtypeStruct((length, groups * STATE), BF16),
            jax.ShapeDtypeStruct((length, groups * STATE), BF16),
            jax.ShapeDtypeStruct((heads, rows), F32),
        ),
        in_specs=[anywhere] + [inside] * 3 + [anywhere] * 4,
        out_specs=[anywhere] * 3 + [inside],
        scratch_shapes=scratch,
        compiler_params=pltpu.CompilerParams(
            collective_id=0, has_side_effects=True, vmem_limit_bytes=60 * 1024 * 1024
        ),
    )(
        layer_input[0],
        dt_weight.T,
        dt_bias[None],
        decay_rate[None],
        ssm_input[0],
        in_basis[0],
        out_basis[0],
        out_cotangent[0],
    )
    return (out_x[None], out_b[None], out_c[None], out_w.T)


def solution(mesh):
    blocks = P("fsdp", "seq", None)
    rows = P("fsdp", None)
    return jax.shard_map(
        body,
        mesh=mesh,
        in_specs=(blocks, rows, P(), P(), blocks, blocks, blocks, blocks),
        out_specs=(blocks, blocks, blocks, rows),
        check_vma=False,
    )
```
